32 devices in a mesh: row: 8 (over z, core), col: 4 (over y, x).
Axes of the slice: x: 2, y: 2, z: 4, core: 2. Of those that a mesh axis runs over, the one named last changes fastest.
Arguments:
- attn_out: bfloat16 [6, 512, 2048], P(None, 'col', 'row'), may hold values from -0.625 to 0.625
- out_cotangent: bfloat16 [6, 512, 2048], P(None, 'row', 'col'), may hold values from -6 to 6
- frozen: bfloat16 [6, 2048, 2048], P(None, 'row', 'col'), may hold values from -0.5 to 0.5
- adapt_in: bfloat16 [6, 32, 2048], P(None, None, 'row'), may hold values from -0.125 to 0.125
- adapt_out: bfloat16 [6, 32, 2048], P(None, None, 'col'), may hold values from -1 to 1
- magnitude: float32 [6, 2048], P(None, 'col'), may hold values from 0.1 to 1.9
Outputs:
- input_grad: bfloat16 [6, 512, 2048], P(None, 'col', 'row')
- adapt_in_grad: float32 [6, 32, 2048], P(None, None, 'row')
- adapt_out_grad: float32 [6, 32, 2048], P(None, None, 'col')
- magnitude_grad: float32 [6, 2048], P(None, 'col')
The draws below stay inside these ranges and needn't reach their ends.
All inputs are finite; a program needn't handle non-finite values.
Results may differ from the reference program's by a relative error of at most 0.0065.
Values may be sent and summed in bfloat16 or wider, within the bound.
A program may use at most 64 MiB of HBM per device.

```python
import jax
import jax.numpy as jnp
from jax import lax

WIDTH = 2048
IN_WIDTH = 2048
RANK = 32
LAYERS = 6
TOKENS = 512


def steps_of(key, extent, shards, smallest, top_value):
    def one(dim, shards_of):
        steps = jax.random.uniform(jax.random.fold_in(jax.random.fold_in(key, 6), dim), (shards_of,), jnp.float32, smallest / len(shards), top_value / len(shards))
        return jnp.repeat(jnp.exp(steps), extent[dim] // shards_of).reshape((-1,) + (1,) * (len(extent) - dim - 1))

    level = one(*shards[0])
    for cut in shards[1:]:
        level = level * one(*cut)
    return level


def gaussian(rng, extent, spread, reach, split=(), kind=jnp.bfloat16):
    level = steps_of(rng, extent, split, -0.22, 0.18) if split else 1.0
    entries = jax.random.normal(rng, extent, jnp.float32) * spread * level
    return jnp.minimum(jnp.maximum(entries, -reach), reach).astype(kind)


def setup_inputs(seed: int = 0) -> dict:
    key_list = jax.random.split(jax.random.key(seed), 7)
    attn_out = gaussian(key_list[0], (LAYERS, TOKENS, IN_WIDTH), (TOKENS ** -0.5), 0.625, ((1, 4), (2, 8)))
    out_cotangent = gaussian(key_list[1], (LAYERS, TOKENS, WIDTH), 1.0, 6.0, ((1, 8), (2, 4)))
    frozen = gaussian(key_list[2], (LAYERS, IN_WIDTH, WIDTH), (IN_WIDTH // 16) ** -0.5, 0.5, ((1, 8), (2, 4)))
    adapt_in = gaussian(key_list[3], (LAYERS, RANK, IN_WIDTH), IN_WIDTH ** -0.5, 0.125, ((2, 8),))
    adapt_out = gaussian(key_list[4], (LAYERS, RANK, WIDTH), RANK ** -0.5, 1.0, ((2, 4),))
    magnitude = jnp.clip(1.0 + 0.18 * jax.random.normal(key_list[5], (LAYERS, WIDTH), jnp.float32), 0.1, 1.9)
    return {"attn_out": attn_out, "out_cotangent": out_cotangent, "frozen": frozen, "adapt_in": adapt_in, "adapt_out": adapt_out, "magnitude": magnitude}


precise = lax.Precision.HIGHEST

def one_layer(acts, grads, frozen, adapt_in, adapt_out, magnitude):
    merged = frozen.astype(jnp.float32) + lax.dot_general(adapt_in, adapt_out, (((0,), (0,)), ((), ())), preferred_element_type=jnp.float32)
    squares = lax.optimization_barrier(jnp.sum(merged * merged, axis=0))
    norms = jnp.sqrt(squares + 0.25)
    outer = lax.dot_general(acts, grads, (((0,), (0,)), ((), ())), preferred_element_type=jnp.float32)
    dots = lax.optimization_barrier(jnp.sum(merged * outer, axis=0))
    scales = magnitude / norms
    correct = -magnitude * dots / (norms * norms * norms)
    magnitude_grad = dots / norms
    delta = outer * scales + merged * correct
    in_grad = lax.dot_general(adapt_out.astype(jnp.float32), delta, (((1,), (1,)), ((), ())), precision=precise)
    out_grad = jnp.dot(adapt_in.astype(jnp.float32), delta, precision=precise)
    scaled = (grads * scales).astype(jnp.bfloat16)
    weight_low = merged.astype(jnp.bfloat16)
    input_grad = lax.dot_general(scaled, weight_low, (((1,), (1,)), ((), ())), preferred_element_type=jnp.float32).astype(jnp.bfloat16)
    return (input_grad, in_grad, out_grad, magnitude_grad)

def reference(attn_out, out_cotangent, frozen, adapt_in, adapt_out, magnitude):
    results = [one_layer(attn_out[layer_at], out_cotangent[layer_at], frozen[layer_at], adapt_in[layer_at], adapt_out[layer_at], magnitude[layer_at]) for layer_at in range(LAYERS)]
    return (jnp.stack([item[0] for item in results]), jnp.stack([item[1] for item in results]), jnp.stack([item[2] for item in results]), jnp.stack([item[3] for item in results]))
```

```python
import functools

import jax
import jax.numpy as jnp
from jax import lax
from jax.experimental import pallas as pl
from jax.experimental.pallas import tpu as pltpu
from jax.sharding import PartitionSpec as P

MESH = pl.DeviceIdType.MESH
F32 = jnp.float32
BF16 = jnp.bfloat16


def mm(a, b, dims):
    return lax.dot_general(a, b, (dims, ((), ())), preferred_element_type=F32)


def kernel(
    R, C,
    acts, grads, frozen, ain, aout, mag,
    ig, ing, oug, mgrad,
    G, A, merged, wlow, prod, own, rs_send, rs_recv,
    sq, dt, im_send, im_recv, io_send, io_recv, og, q, q_recv,
    scl, cor, send, g_in, g_fw, a_in, rs_in, sq_in, dt_in, im_in, io_in, og_in, q_in,
):
    L, TR, W = grads.shape
    TC, KI = acts.shape[1:]
    RANK = ain.shape[1]
    k = RANK // R
    Z = R // 2
    r, c = lax.axis_index("row"), lax.axis_index("col")
    z, core = r // 2, lax.rem(r, 2)
    sib = 2 * z + 1 - core

    def row_to(d):
        return lax.rem(r + d, R)

    def row_from(d):
        return lax.rem(r + R - d, R)

    def col_to(d):
        return lax.rem(c + d, C)

    def z_to(d):
        return 2 * lax.rem(z + d, Z) + core

    def z_from(d):
        return 2 * lax.rem(z + Z - d, Z) + core

    def rows(at, size):
        return pl.ds(pl.multiple_of(at * size, size), size)

    def rcopy(src, dst, cat, recv, **dev):
        return pltpu.make_async_remote_copy(
            src_ref=src, dst_ref=dst, send_sem=send.at[cat], recv_sem=recv,
            device_id=dev, device_id_type=MESH,
        )

    barrier = pltpu.get_barrier_semaphore()
    for d in range(1, R):
        pl.semaphore_signal(barrier, inc=1, device_id={"row": row_to(d)}, device_id_type=MESH)
    for d in range(1, C):
        pl.semaphore_signal(barrier, inc=1, device_id={"col": col_to(d)}, device_id_type=MESH)
    pl.semaphore_wait(barrier, R + C - 2)

    def g_copy(l, d):
        peer = sib if d == 0 else z_to(d)
        return rcopy(grads.at[l], G.at[l, rows(r, TR)], 0, g_in.at[l, d], row=peer)

    def a_copy(l, d):
        return rcopy(acts.at[l], A.at[l, rows(c, TC)], 1, a_in.at[l, d], col=col_to(d))

    def fw_copy(l, d):
        block = G.at[l, rows(z_from(d), TR)]
        return rcopy(block, block, 2, g_fw.at[l, d], row=sib)

    def rs_copy(l, d):
        return rcopy(rs_send.at[d, l], rs_recv.at[d, l], 3, rs_in.at[l, d], col=col_to(d))

    def sq_copy(d):
        return rcopy(sq.at[r], sq.at[r], 4, sq_in.at[d], row=row_to(d))

    def dt_copy(d):
        return rcopy(dt.at[r], dt.at[r], 5, dt_in.at[d], row=row_to(d))

    def im_copy(d):
        return rcopy(im_send.at[row_to(d)], im_recv.at[r], 6, im_in.at[d], row=row_to(d))

    def io_copy(d):
        return rcopy(io_send.at[row_to(d)], io_recv.at[r], 7, io_in.at[d], row=row_to(d))

    def og_copy(d):
        return rcopy(og.at[r], og.at[r], 8, og_in.at[d], row=row_to(d))

    def q_copy(d):
        return rcopy(q, q_recv.at[d], 9, q_in.at[d], col=col_to(d))

    @pl.loop(0, L)
    def _(l):
        for d in range(Z):
            g_copy(l, d).start()
        for d in range(1, C):
            a_copy(l, d).start()

    @pl.loop(0, L)
    def _(l):
        G[l, rows(r, TR)] = grads[l]
        A[l, rows(c, TC)] = acts[l]
        m = frozen[l].astype(F32) + mm(ain[l], aout[l], ((0,), (0,)))
        merged[l] = m
        low = m.astype(BF16)
        wlow[l] = low
        sq[r, l] = jnp.sum(m * m, axis=0, keepdims=True)
        inner = mm(ain[l], low, ((1,), (0,)))
        for s in range(R):
            im_send[s, l] = inner[s * k:(s + 1) * k]

    for d in range(1, R):
        sq_copy(d).start()
    for d in range(1, R):
        im_copy(d).start()
    im_recv[r] = im_send[r]
    for d in range(1, R):
        rcopy(sq.at[r], sq.at[row_from(d)], 4, sq_in.at[d], row=r).wait_recv()
    total = sq[0]
    for s in range(1, R):
        total = total + sq[s]
    scl[...] = mag[...] / jnp.sqrt(total + 0.25)

    @pl.loop(0, L)
    def _(l):
        for d in range(1, Z):
            rcopy(grads.at[l], G.at[l, rows(z_from(d), TR)], 0, g_in.at[l, d], row=r).wait_recv()
            fw_copy(l, d).start()
        rcopy(grads.at[l], G.at[l, rows(sib, TR)], 0, g_in.at[l, 0], row=r).wait_recv()
        for d in range(1, Z):
            from_sib = 2 * lax.rem(z + Z - d, Z) + 1 - core
            rcopy(grads.at[l], G.at[l, rows(from_sib, TR)], 2, g_fw.at[l, d], row=r).wait_recv()
        scale = scl[l]
        g = G[l]
        scaled = (g.astype(F32) * scale).astype(BF16)
        prod[...] = mm(scaled, wlow[l], ((1,), (1,)))
        for d in range(1, C):
            rs_send[d, l] = prod[rows(col_to(d), TC)].astype(BF16)
            rs_copy(l, d).start()
        own[l] = prod[rows(c, TC)]
        for d in range(1, C):
            src = lax.rem(c + C - d, C)
            rcopy(acts.at[l], A.at[l, rows(src, TC)], 1, a_in.at[l, d], col=c).wait_recv()
        outer = mm(A[l], g, ((0,), (0,)))
        dt[r, l] = jnp.sum(merged[l] * outer, axis=0, keepdims=True)
        inner = mm(ain[l], outer.astype(BF16), ((1,), (0,)))
        for s in range(R):
            io_send[s, l] = inner[s * k:(s + 1) * k]
        ing[l] = mm(aout[l], (outer * scale).astype(BF16), ((1,), (1,)))

    for d in range(1, R):
        dt_copy(d).start()
    for d in range(1, R):
        io_copy(d).start()
    io_recv[r] = io_send[r]
    for d in range(1, R):
        rcopy(dt.at[r], dt.at[row_from(d)], 5, dt_in.at[d], row=r).wait_recv()
    dots = dt[0]
    for s in range(1, R):
        dots = dots + dt[s]
    norms = jnp.sqrt(total + 0.25)
    mgrad[...] = dots / norms
    cor[...] = -mag[...] * dots / (norms * norms * norms)

    @pl.loop(0, L)
    def _(l):
        adjusted = (merged[l] * cor[l]).astype(BF16)
        part = ing[l] + mm(aout[l], adjusted, ((1,), (1,)))
        ing[l] = part
        q[l] = part.astype(BF16)

    for d in range(1, C):
        q_copy(d).start()
    for d in range(1, R):
        rcopy(im_recv.at[r], im_recv.at[row_from(d)], 6, im_in.at[d], row=r).wait_recv()
        rcopy(io_recv.at[r], io_recv.at[row_from(d)], 7, io_in.at[d], row=r).wait_recv()

    @pl.loop(0, L)
    def _(l):
        summed, side = io_recv[0, l], im_recv[0, l]
        for s in range(1, R):
            summed = summed + io_recv[s, l]
            side = side + im_recv[s, l]
        og[r, l] = summed * scl[l] + side * cor[l]

    for d in range(1, R):
        og_copy(d).start()

    @pl.loop(0, L)
    def _(l):
        result = own[l]
        for d in range(1, C):
            rcopy(rs_send.at[d, l], rs_recv.at[d, l], 3, rs_in.at[l, d], col=c).wait_recv()
            result = result + rs_recv[d, l].astype(F32)
        ig[l] = result.astype(BF16)

    for d in range(1, C):
        rcopy(q, q_recv.at[d], 9, q_in.at[d], col=c).wait_recv()

    @pl.loop(0, L)
    def _(l):
        result = ing[l]
        for d in range(1, C):
            result = result + q_recv[d, l].astype(F32)
        ing[l] = result

    for d in range(1, R):
        rcopy(og.at[r], og.at[row_from(d)], 8, og_in.at[d], row=r).wait_recv()

    @pl.loop(0, L)
    def _(l):
        for s in range(R):
            oug[l, s * k:(s + 1) * k] = og[s, l]

    @pl.loop(0, L)
    def _(l):
        for d in range(Z):
            g_copy(l, d).wait_send()
        for d in range(1, Z):
            fw_copy(l, d).wait_send()
        for d in range(1, C):
            a_copy(l, d).wait_send()
            rs_copy(l, d).wait_send()

    for d in range(1, R):
        sq_copy(d).wait_send()
        im_copy(d).wait_send()
        dt_copy(d).wait_send()
        io_copy(d).wait_send()
        og_copy(d).wait_send()
    for d in range(1, C):
        q_copy(d).wait_send()


def body(R, C, acts, grads, frozen, ain, aout, mag):
    L, TR, W = grads.shape
    TC, KI = acts.shape[1:]
    RANK = ain.shape[1]
    k, T, Z = RANK // R, TR * R, R // 2
    V = pltpu.VMEM
    dma = pltpu.SemaphoreType.DMA
    vm = pl.BlockSpec(memory_space=pltpu.VMEM)
    ig, ing, oug, mgrad = pl.pallas_call(
        functools.partial(kernel, R, C),
        out_shape=(
            jax.ShapeDtypeStruct((L, TC, KI), BF16),
            jax.ShapeDtypeStruct((L, RANK, KI), F32),
            jax.ShapeDtypeStruct((L, RANK, W), F32),
            jax.ShapeDtypeStruct((L, 1, W), F32),
        ),
        in_specs=[vm] * 6,
        out_specs=(vm,) * 4,
        scratch_shapes=[
            V((L, T, W), BF16), V((L, T, KI), BF16), V((L, KI, W), F32), V((L, KI, W), BF16),
            V((T, KI), F32), V((L, TC, KI), F32), V((C, L, TC, KI), BF16), V((C, L, TC, KI), BF16),
            V((R, L, 1, W), F32), V((R, L, 1, W), F32),
            V((R, L, k, W), F32), V((R, L, k, W), F32), V((R, L, k, W), F32), V((R, L, k, W), F32),
            V((R, L, k, W), F32), V((L, RANK, KI), BF16), V((C, L, RANK, KI), BF16),
            V((L, 1, W), F32), V((L, 1, W), F32),
            dma((10,)), dma((L, Z)), dma((L, Z)), dma((L, C)), dma((L, C)),
            dma((R,)), dma((R,)), dma((R,)), dma((R,)), dma((R,)), dma((C,)),
        ],
        compiler_params=pltpu.CompilerParams(
            collective_id=0, has_side_effects=True, vmem_limit_bytes=60 * 1024 * 1024
        ),
    )(acts, grads, frozen, ain, aout, mag[:, None, :])
    return ig, ing, oug, mgrad[:, 0, :]


def solution(mesh):
    return jax.shard_map(
        functools.partial(body, mesh.shape["row"], mesh.shape["col"]),
        mesh=mesh,
        in_specs=(
            P(None, "col", "row"),
            P(None, "row", "col"),
            P(None, "row", "col"),
            P(None, None, "row"),
            P(None, None, "col"),
            P(None, "col"),
        ),
        out_specs=(
            P(None, "col", "row"),
            P(None, None, "row"),
            P(None, None, "col"),
            P(None, "col"),
        ),
        check_vma=False,
    )
```

```python
import functools

import jax
import jax.numpy as jnp
from jax import lax
from jax.experimental import pallas as pl
from jax.experimental.pallas import tpu as pltpu
from jax.sharding import PartitionSpec as P

MESH = pl.DeviceIdType.MESH
F32 = jnp.float32
BF16 = jnp.bfloat16


def mm(a, b, dims):
    return lax.dot_general(a, b, (dims, ((), ())), preferred_element_type=F32)


def kernel(
    R, C,
    acts, grads, frozen, ain, aout, mag,
    ig, ing, oug, mgrad,
    G, A, merged, wlow, prod, own, rs_send, rs_recv,
    sq, dt, im_send, im_sib, im_acc, im_recv, io_send, io_sib, io_acc, io_recv, og, q, q_recv,
    scl, cor, mag3, send, g_in, g_fw, a_in, rs_in, sq_in, dt_in, im_in, io_in, io_fw, og_in, og_fw, q_in,
):
    L, TR, W = grads.shape
    TC, KI = acts.shape[1:]
    RANK = ain.shape[1]
    k = RANK // R
    Z = R // 2
    r, c = lax.axis_index("row"), lax.axis_index("col")
    z, core = r // 2, lax.rem(r, 2)
    sib = 2 * z + 1 - core

    def row_to(d):
        return lax.rem(r + d, R)

    def row_from(d):
        return lax.rem(r + R - d, R)

    def col_to(d):
        return lax.rem(c + d, C)

    def z_to(d):
        return 2 * lax.rem(z + d, Z) + core

    def z_from(d):
        return 2 * lax.rem(z + Z - d, Z) + core

    def rows(at, size):
        return pl.ds(pl.multiple_of(at * size, size), size)

    def rcopy(src, dst, cat, recv, **dev):
        return pltpu.make_async_remote_copy(
            src_ref=src, dst_ref=dst, send_sem=send.at[cat], recv_sem=recv,
            device_id=dev, device_id_type=MESH,
        )

    barrier = pltpu.get_barrier_semaphore()
    for d in range(1, R):
        pl.semaphore_signal(barrier, inc=1, device_id={"row": row_to(d)}, device_id_type=MESH)
    for d in range(1, C):
        pl.semaphore_signal(barrier, inc=1, device_id={"col": col_to(d)}, device_id_type=MESH)
    pl.semaphore_wait(barrier, R + C - 2)

    def g_copy(l, d):
        peer = sib if d == 0 else z_to(d)
        return rcopy(grads.at[l], G.at[l, rows(r, TR)], 0, g_in.at[l, d], row=peer)

    def a_copy(l, d):
        return rcopy(acts.at[l], A.at[l, rows(c, TC)], 1, a_in.at[l, d], col=col_to(d))

    def fw_copy(l, d):
        block = G.at[l, rows(z_from(d), TR)]
        return rcopy(block, block, 2, g_fw.at[l, d], row=sib)

    def rs_copy(l, d):
        return rcopy(rs_send.at[d, l], rs_recv.at[d, l], 3, rs_in.at[l, d], col=col_to(d))

    def sq_copy(d):
        return rcopy(sq.at[r], sq.at[r], 4, sq_in.at[d], row=row_to(d))

    def dt_copy(l, d):
        return rcopy(dt.at[r, l], dt.at[r, l], 5, dt_in.at[l, d], row=row_to(d))

    def at_z(d):
        return lax.rem(z + d, Z)

    def im_copy(d):
        if d == 0:
            return rcopy(im_send.at[1 - core], im_sib, 6, im_in.at[0], row=sib)
        return rcopy(im_acc.at[at_z(d)], im_recv.at[z], 7, im_in.at[d], row=z_to(d))

    def io_fw_copy(l):
        return rcopy(io_send.at[1 - core, l], io_sib.at[l], 8, io_fw.at[l], row=sib)

    def io_copy(l, d):
        return rcopy(io_acc.at[at_z(d), l], io_recv.at[z, l], 9, io_in.at[l, d], row=z_to(d))

    def og_copy(d):
        return rcopy(og.at[r], og.at[r], 11, og_in.at[d], row=sib if d == 0 else z_to(d))

    def og_fw_copy(d):
        return rcopy(og.at[z_from(d)], og.at[z_from(d)], 12, og_fw.at[d], row=sib)

    def q_copy(d):
        return rcopy(q, q_recv.at[d], 10, q_in.at[d], col=col_to(d))

    @pl.loop(0, L)
    def _(l):
        for d in range(Z):
            g_copy(l, d).start()
        for d in range(1, C):
            a_copy(l, d).start()

    @pl.loop(0, L)
    def _(l):
        G[l, rows(r, TR)] = grads[l]
        A[l, rows(c, TC)] = acts[l]
        m = frozen[l].astype(F32) + mm(ain[l], aout[l], ((0,), (0,)))
        merged[l] = m
        low = m.astype(BF16)
        wlow[l] = low
        sq[r, l] = jnp.sum(m * m, axis=0, keepdims=True)
        inner = mm(ain[l], low, ((1,), (0,)))
        for s in range(R):
            im_send[s % 2, s // 2, l] = inner[s * k:(s + 1) * k]

    for d in range(1, R):
        sq_copy(d).start()
    im_copy(0).start()
    for l in range(L):
        mag3[l] = mag[l:l + 1]
    for d in range(1, R):
        rcopy(sq.at[r], sq.at[row_from(d)], 4, sq_in.at[d], row=r).wait_recv()
    total = sq[0]
    for s in range(1, R):
        total = total + sq[s]
    scl[...] = mag3[...] / jnp.sqrt(total + 0.25)
    im_copy(0).wait_recv()
    im_acc[...] = im_send[core] + im_sib[...]
    for d in range(1, Z):
        im_copy(d).start()
    im_recv[z] = im_acc[z]

    def pass_on(l):
        rcopy(io_sib.at[l], io_sib.at[l], 8, io_fw.at[l], row=sib).wait_recv()
        for s in range(Z):
            io_acc[s, l] = io_send[core, l, s] + io_sib[l, s]
        for d in range(1, Z):
            io_copy(l, d).start()
        io_recv[z, l] = io_acc[z, l]

    @pl.loop(0, L)
    def _(l):
        for d in range(1, Z):
            rcopy(grads.at[l], G.at[l, rows(z_from(d), TR)], 0, g_in.at[l, d], row=r).wait_recv()
            fw_copy(l, d).start()
        rcopy(grads.at[l], G.at[l, rows(sib, TR)], 0, g_in.at[l, 0], row=r).wait_recv()
        for d in range(1, Z):
            from_sib = 2 * lax.rem(z + Z - d, Z) + 1 - core
            rcopy(grads.at[l], G.at[l, rows(from_sib, TR)], 2, g_fw.at[l, d], row=r).wait_recv()
        scale = scl[l]
        g = G[l]
        scaled = (g.astype(F32) * scale).astype(BF16)
        prod[...] = mm(scaled, wlow[l], ((1,), (1,)))
        for d in range(1, C):
            rs_send[d, l] = prod[rows(col_to(d), TC)].astype(BF16)
            rs_copy(l, d).start()
        own[l] = prod[rows(c, TC)]
        for d in range(1, C):
            src = lax.rem(c + C - d, C)
            rcopy(acts.at[l], A.at[l, rows(src, TC)], 1, a_in.at[l, d], col=c).wait_recv()
        outer = mm(A[l], g, ((0,), (0,)))
        dt[r, l] = jnp.sum(merged[l] * outer, axis=0, keepdims=True)
        for d in range(1, R):
            dt_copy(l, d).start()
        inner = mm(ain[l], outer.astype(BF16), ((1,), (0,)))
        for s in range(R):
            io_send[s % 2, l, s // 2] = inner[s * k:(s + 1) * k]
        io_fw_copy(l).start()

        @pl.when(l > 0)
        def _():
            pass_on(l - 1)

        ing[l] = mm(aout[l], (outer * scale).astype(BF16), ((1,), (1,)))

    pass_on(L - 1)

    @pl.loop(0, L)
    def _(l):
        for d in range(1, R):
            rcopy(dt.at[r, l], dt.at[row_from(d), l], 5, dt_in.at[l, d], row=r).wait_recv()

    dots = dt[0]
    for s in range(1, R):
        dots = dots + dt[s]
    norms = jnp.sqrt(total + 0.25)
    ratio = dots / norms
    for l in range(L):
        mgrad[l:l + 1] = ratio[l]
    cor[...] = -mag3[...] * dots / (norms * norms * norms)

    @pl.loop(0, L)
    def _(l):
        adjusted = (merged[l] * cor[l]).astype(BF16)
        part = ing[l] + mm(aout[l], adjusted, ((1,), (1,)))
        ing[l] = part
        q[l] = part.astype(BF16)

    for d in range(1, C):
        q_copy(d).start()
    for d in range(1, Z):
        src = lax.rem(z + Z - d, Z)
        rcopy(im_recv.at[z], im_recv.at[src], 7, im_in.at[d], row=r).wait_recv()

    @pl.loop(0, L)
    def _(l):
        for d in range(1, Z):
            src = lax.rem(z + Z - d, Z)
            rcopy(io_recv.at[z, l], io_recv.at[src, l], 9, io_in.at[l, d], row=r).wait_recv()
        summed, side = io_recv[0, l], im_recv[0, l]
        for s in range(1, Z):
            summed = summed + io_recv[s, l]
            side = side + im_recv[s, l]
        og[r, l] = summed * scl[l] + side * cor[l]

    for d in range(Z):
        og_copy(d).start()

    @pl.loop(0, L)
    def _(l):
        result = own[l]
        for d in range(1, C):
            rcopy(rs_send.at[d, l], rs_recv.at[d, l], 3, rs_in.at[l, d], col=c).wait_recv()
            result = result + rs_recv[d, l].astype(F32)
        ig[l] = result.astype(BF16)

    for d in range(1, C):
        rcopy(q, q_recv.at[d], 10, q_in.at[d], col=c).wait_recv()

    @pl.loop(0, L)
    def _(l):
        result = ing[l]
        for d in range(1, C):
            result = result + q_recv[d, l].astype(F32)
        ing[l] = result

    for d in range(1, Z):
        rcopy(og.at[r], og.at[z_from(d)], 11, og_in.at[d], row=r).wait_recv()
        og_fw_copy(d).start()
    rcopy(og.at[r], og.at[sib], 11, og_in.at[0], row=r).wait_recv()
    for d in range(1, Z):
        from_sib = 2 * lax.rem(z + Z - d, Z) + 1 - core
        rcopy(og.at[r], og.at[from_sib], 12, og_fw.at[d], row=r).wait_recv()

    @pl.loop(0, L)
    def _(l):
        for s in range(R):
            oug[l, s * k:(s + 1) * k] = og[s, l]

    @pl.loop(0, L)
    def _(l):
        for d in range(Z):
            g_copy(l, d).wait_send()
        for d in range(1, Z):
            fw_copy(l, d).wait_send()
        for d in range(1, C):
            a_copy(l, d).wait_send()
            rs_copy(l, d).wait_send()

    @pl.loop(0, L)
    def _(l):
        for d in range(1, R):
            dt_copy(l, d).wait_send()
        io_fw_copy(l).wait_send()
        for d in range(1, Z):
            io_copy(l, d).wait_send()

    for d in range(1, R):
        sq_copy(d).wait_send()
    for d in range(Z):
        im_copy(d).wait_send()
        og_copy(d).wait_send()
    for d in range(1, Z):
        og_fw_copy(d).wait_send()
    for d in range(1, C):
        q_copy(d).wait_send()


def finish(ig, ing, oug, mgrad, ig_out, ing_out, oug_out, mgrad_out):
    ig_out[...] = ig[...]
    ing_out[...] = ing[...]
    oug_out[...] = oug[...]
    mgrad_out[...] = mgrad[...]


def body(R, C, acts, grads, frozen, ain, aout, mag):
    L, TR, W = grads.shape
    TC, KI = acts.shape[1:]
    RANK = ain.shape[1]
    k, T, Z = RANK // R, TR * R, R // 2
    V = pltpu.VMEM
    dma = pltpu.SemaphoreType.DMA
    vm = pl.BlockSpec(memory_space=pltpu.VMEM)
    ig, ing, oug, mgrad = pl.pallas_call(
        functools.partial(kernel, R, C),
        out_shape=(
            jax.ShapeDtypeStruct((L, TC, KI), BF16),
            jax.ShapeDtypeStruct((L, RANK, KI), F32),
            jax.ShapeDtypeStruct((L, RANK, W), F32),
            jax.ShapeDtypeStruct((L, W), F32),
        ),
        in_specs=[vm] * 6,
        out_specs=(vm,) * 4,
        scratch_shapes=[
            V((L, T, W), BF16), V((L, T, KI), BF16), V((L, KI, W), F32), V((L, KI, W), BF16),
            V((T, KI), F32), V((L, TC, KI), F32), V((C, L, TC, KI), BF16), V((C, L, TC, KI), BF16),
            V((R, L, 1, W), F32), V((R, L, 1, W), F32),
            V((2, Z, L, k, W), F32), V((Z, L, k, W), F32), V((Z, L, k, W), F32), V((Z, L, k, W), F32),
            V((2, L, Z, k, W), F32), V((L, Z, k, W), F32), V((Z, L, k, W), F32), V((Z, L, k, W), F32),
            V((R, L, k, W), F32), V((L, RANK, KI), BF16), V((C, L, RANK, KI), BF16),
            V((L, 1, W), F32), V((L, 1, W), F32), V((L, 1, W), F32),
            dma((13,)), dma((L, Z)), dma((L, Z)), dma((L, C)), dma((L, C)),
            dma((R,)), dma((L, R)), dma((Z,)), dma((L, Z)), dma((L,)), dma((Z,)), dma((Z,)), dma((C,)),
        ],
        compiler_params=pltpu.CompilerParams(
            collective_id=0, has_side_effects=True, vmem_limit_bytes=44 * 1024 * 1024
        ),
    )(acts, grads, frozen, ain, aout, mag)
    return pl.pallas_call(
        finish,
        out_shape=tuple(jax.ShapeDtypeStruct(x.shape, x.dtype) for x in (ig, ing, oug, mgrad)),
        in_specs=[vm] * 4,
        out_specs=(vm,) * 4,
    )(ig, ing, oug, mgrad)


def solution(mesh):
    return jax.shard_map(
        functools.partial(body, mesh.shape["row"], mesh.shape["col"]),
        mesh=mesh,
        in_specs=(
            P(None, "col", "row"),
            P(None, "row", "col"),
            P(None, "row", "col"),
            P(None, None, "row"),
            P(None, None, "col"),
            P(None, "col"),
        ),
        out_specs=(
            P(None, "col", "row"),
            P(None, None, "row"),
            P(None, None, "col"),
            P(None, "col"),
        ),
        check_vma=False,
    )
```

```python
import functools

import jax
import jax.numpy as jnp
from jax import lax
from jax.experimental import pallas as pl
from jax.experimental.pallas import tpu as pltpu
from jax.sharding import PartitionSpec as P

MESH = pl.DeviceIdType.MESH
F32 = jnp.float32
BF16 = jnp.bfloat16


def mm(a, b, dims):
    return lax.dot_general(a, b, (dims, ((), ())), preferred_element_type=F32)


def kernel(
    R, C,
    acts_hbm, grads_hbm, frozen_hbm, ain_hbm, aout_hbm, mag_hbm,
    ig_hbm, ing_hbm, oug_hbm, mgrad_hbm,
    acts, grads, frozen, ain, aout, mag,
    ig, ing, oug, mgrad, load, save,
    G, A, merged, wlow, prod, own, rs_send, rs_recv,
    sq, dt, im_send, im_sib, im_acc, im_recv, io_send, io_sib, io_acc, io_recv, og, q, q_recv,
    scl, cor, mag3, send, g_in, g_fw, a_in, rs_in, sq_in, dt_in, im_in, io_in, io_fw, og_in, og_fw, q_in,
):
    pairs = ((grads_hbm, grads), (acts_hbm, acts), (frozen_hbm, frozen),
             (ain_hbm, ain), (aout_hbm, aout), (mag_hbm, mag))
    loads = [pltpu.make_async_copy(a, b, load.at[i]) for i, (a, b) in enumerate(pairs)]
    for copy in loads:
        copy.start()
    pairs = ((mgrad, mgrad_hbm), (ig, ig_hbm), (ing, ing_hbm), (oug, oug_hbm))
    saves = [pltpu.make_async_copy(a, b, save.at[i]) for i, (a, b) in enumerate(pairs)]
    L, TR, W = grads.shape
    TC, KI = acts.shape[1:]
    RANK = ain.shape[1]
    k = RANK // R
    Z = R // 2
    ahead = min(4, L)
    r, c = lax.axis_index("row"), lax.axis_index("col")
    z, core = r // 2, lax.rem(r, 2)
    sib = 2 * z + 1 - core

    def row_to(d):
        return lax.rem(r + d, R)

    def row_from(d):
        return lax.rem(r + R - d, R)

    def col_to(d):
        return lax.rem(c + d, C)

    def z_to(d):
        return 2 * lax.rem(z + d, Z) + core

    def z_from(d):
        return 2 * lax.rem(z + Z - d, Z) + core

    def rows(at, size):
        return pl.ds(pl.multiple_of(at * size, size), size)

    def rcopy(src, dst, cat, recv, **dev):
        return pltpu.make_async_remote_copy(
            src_ref=src, dst_ref=dst, send_sem=send.at[cat], recv_sem=recv,
            device_id=dev, device_id_type=MESH,
        )

    barrier = pltpu.get_barrier_semaphore()
    for d in range(1, R):
        pl.semaphore_signal(barrier, inc=1, device_id={"row": row_to(d)}, device_id_type=MESH)
    for d in range(1, C):
        pl.semaphore_signal(barrier, inc=1, device_id={"col": col_to(d)}, device_id_type=MESH)
    pl.semaphore_wait(barrier, R + C - 2)

    def g_block(l, at, which):
        return G.at[l, rows(2 * at + which, TR)]

    def g_own(l, step):
        if step == 0:
            return rcopy(grads.at[l], g_block(l, z, core), 2, g_fw.at[l, z], row=sib)
        return rcopy(grads.at[l], g_block(l, z, core), 0, g_in.at[l, z], row=r + 2 * step)

    def g_pass(l, at, step):
        block = g_block(l, at, core)
        if step == 0:
            return rcopy(block, block, 2, g_fw.at[l, at], row=sib)
        return rcopy(block, block, 0, g_in.at[l, at], row=r + 2 * step)

    def g_own_each(l, act):
        act(g_own(l, 0))

        @pl.when(z < Z - 1)
        def _():
            act(g_own(l, 1))

        @pl.when(z > 0)
        def _():
            act(g_own(l, -1))

    def g_relay(l, d, act, arrive):
        for step in (1, -1):
            at = z - step * d

            @pl.when(jnp.logical_and(at >= 0, at < Z))
            def _():
                if arrive:
                    rcopy(grads.at[l], g_block(l, at, core), 0, g_in.at[l, at], row=r).wait_recv()

                @pl.when(jnp.logical_and(z + step >= 0, z + step < Z))
                def _():
                    act(g_pass(l, at, step))

                act(g_pass(l, at, 0))

    def a_copy(l, d):
        return rcopy(acts.at[l], A.at[l, rows(c, TC)], 1, a_in.at[l, d], col=col_to(d))

    def rs_copy(l, d):
        return rcopy(rs_send.at[d, l], rs_recv.at[d, l], 3, rs_in.at[l, d], col=col_to(d))

    def sq_copy(d):
        return rcopy(sq.at[r], sq.at[r], 4, sq_in.at[d], row=row_to(d))

    def dt_copy(l, d):
        return rcopy(dt.at[r, l], dt.at[r, l], 5, dt_in.at[l, d], row=row_to(d))

    def at_z(d):
        return lax.rem(z + d, Z)

    def im_copy(d):
        if d == 0:
            return rcopy(im_send.at[1 - core], im_sib, 6, im_in.at[0], row=sib)
        return rcopy(im_acc.at[at_z(d)], im_recv.at[z], 7, im_in.at[d], row=z_to(d))

    def io_fw_copy(l):
        return rcopy(io_send.at[1 - core, l], io_sib.at[l], 8, io_fw.at[l], row=sib)

    def io_copy(l, d):
        return rcopy(io_acc.at[at_z(d), l], io_recv.at[z, l], 9, io_in.at[l, d], row=z_to(d))

    def og_copy(d):
        return rcopy(og.at[r], og.at[r], 11, og_in.at[d], row=sib if d == 0 else z_to(d))

    def og_fw_copy(d):
        return rcopy(og.at[z_from(d)], og.at[z_from(d)], 12, og_fw.at[d], row=sib)

    def q_copy(d):
        return rcopy(q, q_recv.at[d], 10, q_in.at[d], col=col_to(d))

    loads[0].wait()
    loads[1].wait()

    @pl.loop(0, L)
    def _(l):
        @pl.when(l < ahead)
        def _():
            g_own_each(l, lambda copy: copy.start())

        for d in range(1, C):
            a_copy(l, d).start()

    for copy in loads[2:]:
        copy.wait()

    @pl.loop(0, L)
    def _(l):
        G[l, rows(r, TR)] = grads[l]
        A[l, rows(c, TC)] = acts[l]
        m = frozen[l].astype(F32) + mm(ain[l], aout[l], ((0,), (0,)))
        merged[l] = m
        low = m.astype(BF16)
        wlow[l] = low
        sq[r, l] = jnp.sum(m * m, axis=0, keepdims=True)
        inner = mm(ain[l], low, ((1,), (0,)))
        for s in range(R):
            im_send[s % 2, s // 2, l] = inner[s * k:(s + 1) * k]

    for d in range(1, R):
        sq_copy(d).start()
    im_copy(0).start()
    for l in range(L):
        mag3[l] = mag[l:l + 1]
    for d in range(1, R):
        rcopy(sq.at[r], sq.at[row_from(d)], 4, sq_in.at[d], row=r).wait_recv()
    total = sq[0]
    for s in range(1, R):
        total = total + sq[s]
    scl[...] = mag3[...] / jnp.sqrt(total + 0.25)
    def pass_on(l):
        rcopy(io_sib.at[l], io_sib.at[l], 8, io_fw.at[l], row=sib).wait_recv()
        for s in range(Z):
            io_acc[s, l] = io_send[core, l, s] + io_sib[l, s]
        for d in range(1, Z):
            io_copy(l, d).start()
        io_recv[z, l] = io_acc[z, l]

    def compute(l):
        for at in range(Z):
            rcopy(grads.at[l], g_block(l, at, 1 - core), 2, g_fw.at[l, at], row=r).wait_recv()
        scale = scl[l]
        g = G[l]
        scaled = (g.astype(F32) * scale).astype(BF16)
        prod[...] = mm(scaled, wlow[l], ((1,), (1,)))
        for d in range(1, C):
            rs_send[d, l] = prod[rows(col_to(d), TC)].astype(BF16)
            rs_copy(l, d).start()
        own[l] = prod[rows(c, TC)]
        for d in range(1, C):
            src = lax.rem(c + C - d, C)
            rcopy(acts.at[l], A.at[l, rows(src, TC)], 1, a_in.at[l, d], col=c).wait_recv()
        outer = mm(A[l], g, ((0,), (0,)))
        dt[r, l] = jnp.sum(merged[l] * outer, axis=0, keepdims=True)
        for d in range(1, R):
            dt_copy(l, d).start()
        inner = mm(ain[l], outer.astype(BF16), ((1,), (0,)))
        for s in range(R):
            io_send[s % 2, l, s // 2] = inner[s * k:(s + 1) * k]
        io_fw_copy(l).start()

        @pl.when(l > 0)
        def _():
            pass_on(l - 1)

        ing[l] = mm(aout[l], (outer * scale).astype(BF16), ((1,), (1,)))

    @pl.loop(0, L + Z - 1)
    def _(at):
        @pl.when(at + ahead < L)
        def _():
            g_own_each(at + ahead, lambda copy: copy.start())

        for d in range(1, Z):
            l = at - (d - 1)

            @pl.when(jnp.logical_and(l >= 0, l < L))
            def _():
                g_relay(l, d, lambda copy: copy.start(), True)

        @pl.when(at == L - 1)
        def _():
            im_copy(0).wait_recv()
            im_acc[...] = im_send[core] + im_sib[...]
            for d in range(1, Z):
                im_copy(d).start()
            im_recv[z] = im_acc[z]

        @pl.when(at >= Z - 1)
        def _():
            compute(at - (Z - 1))

    pass_on(L - 1)

    @pl.loop(0, L)
    def _(l):
        for d in range(1, R):
            rcopy(dt.at[r, l], dt.at[row_from(d), l], 5, dt_in.at[l, d], row=r).wait_recv()

    dots = dt[0]
    for s in range(1, R):
        dots = dots + dt[s]
    norms = jnp.sqrt(total + 0.25)
    ratio = dots / norms
    for l in range(L):
        mgrad[l:l + 1] = ratio[l]
    saves[0].start()
    cor[...] = -mag3[...] * dots / (norms * norms * norms)

    @pl.loop(0, L)
    def _(l):
        adjusted = (merged[l] * cor[l]).astype(BF16)
        part = ing[l] + mm(aout[l], adjusted, ((1,), (1,)))
        ing[l] = part
        q[l] = part.astype(BF16)

    for d in range(1, C):
        q_copy(d).start()
    for d in range(1, Z):
        src = lax.rem(z + Z - d, Z)
        rcopy(im_recv.at[z], im_recv.at[src], 7, im_in.at[d], row=r).wait_recv()

    @pl.loop(0, L)
    def _(l):
        for d in range(1, Z):
            src = lax.rem(z + Z - d, Z)
            rcopy(io_recv.at[z, l], io_recv.at[src, l], 9, io_in.at[l, d], row=r).wait_recv()
        summed, side = io_recv[0, l], im_recv[0, l]
        for s in range(1, Z):
            summed = summed + io_recv[s, l]
            side = side + im_recv[s, l]
        og[r, l] = summed * scl[l] + side * cor[l]

    for d in range(Z):
        og_copy(d).start()

    @pl.loop(0, L)
    def _(l):
        result = own[l]
        for d in range(1, C):
            rcopy(rs_send.at[d, l], rs_recv.at[d, l], 3, rs_in.at[l, d], col=c).wait_recv()
            result = result + rs_recv[d, l].astype(F32)
        ig[l] = result.astype(BF16)

    saves[1].start()

    for d in range(1, C):
        rcopy(q, q_recv.at[d], 10, q_in.at[d], col=c).wait_recv()

    @pl.loop(0, L)
    def _(l):
        result = ing[l]
        for d in range(1, C):
            result = result + q_recv[d, l].astype(F32)
        ing[l] = result

    saves[2].start()

    for d in range(1, Z):
        rcopy(og.at[r], og.at[z_from(d)], 11, og_in.at[d], row=r).wait_recv()
        og_fw_copy(d).start()
    rcopy(og.at[r], og.at[sib], 11, og_in.at[0], row=r).wait_recv()
    for d in range(1, Z):
        from_sib = 2 * lax.rem(z + Z - d, Z) + 1 - core
        rcopy(og.at[r], og.at[from_sib], 12, og_fw.at[d], row=r).wait_recv()

    @pl.loop(0, L)
    def _(l):
        for s in range(R):
            oug[l, s * k:(s + 1) * k] = og[s, l]

    saves[3].start()

    @pl.loop(0, L)
    def _(l):
        g_own_each(l, lambda copy: copy.wait_send())
        for d in range(1, Z):
            g_relay(l, d, lambda copy: copy.wait_send(), False)
        for d in range(1, C):
            a_copy(l, d).wait_send()
            rs_copy(l, d).wait_send()

    @pl.loop(0, L)
    def _(l):
        for d in range(1, R):
            dt_copy(l, d).wait_send()
        io_fw_copy(l).wait_send()
        for d in range(1, Z):
            io_copy(l, d).wait_send()

    for d in range(1, R):
        sq_copy(d).wait_send()
    for d in range(Z):
        im_copy(d).wait_send()
        og_copy(d).wait_send()
    for d in range(1, Z):
        og_fw_copy(d).wait_send()
    for d in range(1, C):
        q_copy(d).wait_send()
    for copy in saves:
        copy.wait()


def finish(ig, ing, oug, mgrad, ig_out, ing_out, oug_out, mgrad_out):
    ig_out[...] = ig[...]
    ing_out[...] = ing[...]
    oug_out[...] = oug[...]
    mgrad_out[...] = mgrad[...]


def body(R, C, acts, grads, frozen, ain, aout, mag):
    L, TR, W = grads.shape
    TC, KI = acts.shape[1:]
    RANK = ain.shape[1]
    k, T, Z = RANK // R, TR * R, R // 2
    V = pltpu.VMEM
    dma = pltpu.SemaphoreType.DMA
    vm = pl.BlockSpec(memory_space=pltpu.VMEM)
    hbm = pl.BlockSpec(memory_space=pltpu.HBM)
    ig, ing, oug, mgrad = pl.pallas_call(
        functools.partial(kernel, R, C),
        out_shape=(
            jax.ShapeDtypeStruct((L, TC, KI), BF16),
            jax.ShapeDtypeStruct((L, RANK, KI), F32),
            jax.ShapeDtypeStruct((L, RANK, W), F32),
            jax.ShapeDtypeStruct((L, W), F32),
        ),
        in_specs=[hbm] * 6,
        out_specs=(hbm,) * 4,
        scratch_shapes=[
            V(acts.shape, BF16), V(grads.shape, BF16), V(frozen.shape, BF16),
            V(ain.shape, BF16), V(aout.shape, BF16), V(mag.shape, F32),
            V((L, TC, KI), BF16), V((L, RANK, KI), F32), V((L, RANK, W), F32), V((L, W), F32),
            dma((6,)), dma((4,)),
            V((L, T, W), BF16), V((L, T, KI), BF16), V((L, KI, W), F32), V((L, KI, W), BF16),
            V((T, KI), F32), V((L, TC, KI), F32), V((C, L, TC, KI), BF16), V((C, L, TC, KI), BF16),
            V((R, L, 1, W), F32), V((R, L, 1, W), F32),
            V((2, Z, L, k, W), F32), V((Z, L, k, W), F32), V((Z, L, k, W), F32), V((Z, L, k, W), F32),
            V((2, L, Z, k, W), F32), V((L, Z, k, W), F32), V((Z, L, k, W), F32), V((Z, L, k, W), F32),
            V((R, L, k, W), F32), V((L, RANK, KI), BF16), V((C, L, RANK, KI), BF16),
            V((L, 1, W), F32), V((L, 1, W), F32), V((L, 1, W), F32),
            dma((13,)), dma((L, Z)), dma((L, Z)), dma((L, C)), dma((L, C)),
            dma((R,)), dma((L, R)), dma((Z,)), dma((L, Z)), dma((L,)), dma((Z,)), dma((Z,)), dma((C,)),
        ],
        compiler_params=pltpu.CompilerParams(
            collective_id=0, has_side_effects=True, vmem_limit_bytes=60 * 1024 * 1024
        ),
    )(acts, grads, frozen, ain, aout, mag)
    return pl.pallas_call(
        finish,
        out_shape=tuple(jax.ShapeDtypeStruct(x.shape, x.dtype) for x in (ig, ing, oug, mgrad)),
        in_specs=[vm] * 4,
        out_specs=(vm,) * 4,
    )(ig, ing, oug, mgrad)


def solution(mesh):
    return jax.shard_map(
        functools.partial(body, mesh.shape["row"], mesh.shape["col"]),
        mesh=mesh,
        in_specs=(
            P(None, "col", "row"),
            P(None, "row", "col"),
            P(None, "row", "col"),
            P(None, None, "row"),
            P(None, None, "col"),
            P(None, "col"),
        ),
        out_specs=(
            P(None, "col", "row"),
            P(None, None, "row"),
            P(None, None, "col"),
            P(None, "col"),
        ),
        check_vma=False,
    )
```

```python
import functools

import jax
import jax.numpy as jnp
from jax import lax
from jax.experimental import pallas as pl
from jax.experimental.pallas import tpu as pltpu
from jax.sharding import PartitionSpec as P

MESH = pl.DeviceIdType.MESH
F32 = jnp.float32
BF16 = jnp.bfloat16


def mm(a, b, dims):
    return lax.dot_general(a, b, (dims, ((), ())), preferred_element_type=F32)


def kernel(
    R, C,
    acts_hbm, grads_hbm, frozen_hbm, ain_hbm, aout_hbm, mag_hbm,
    ig_hbm, ing_hbm, oug_hbm, mgrad_hbm,
    acts, grads, frozen, ain, aout, mag,
    ig, ing, oug, mgrad, load, save,
    G, A, merged, wlow, prod, own, rs_send, rs_recv,
    sq, dt, im_send, im_sib, im_acc, im_recv, io_send, io_sib, io_acc, io_recv, og, q, q_recv,
    scl, cor, mag3, send, g_in, g_fw, a_in, rs_in, sq_in, dt_in, im_in, io_in, io_fw, og_in, og_fw, q_in,
):
    pairs = ((grads_hbm, grads), (acts_hbm, acts), (frozen_hbm, frozen),
             (ain_hbm, ain), (aout_hbm, aout), (mag_hbm, mag))
    loads = [pltpu.make_async_copy(a, b, load.at[i]) for i, (a, b) in enumerate(pairs)]
    for copy in loads:
        copy.start()
    pairs = ((mgrad, mgrad_hbm), (ig, ig_hbm), (ing, ing_hbm), (oug, oug_hbm))
    saves = [pltpu.make_async_copy(a, b, save.at[i]) for i, (a, b) in enumerate(pairs)]
    L, TR, W = grads.shape
    TC, KI = acts.shape[1:]
    RANK = ain.shape[1]
    k = RANK // R
    Z = R // 2
    ahead = min(3, L)
    skew = (Z - 2) // 2
    r, c = lax.axis_index("row"), lax.axis_index("col")
    z, core = r // 2, lax.rem(r, 2)
    sib = 2 * z + 1 - core

    def row_to(d):
        return lax.rem(r + d, R)

    def row_from(d):
        return lax.rem(r + R - d, R)

    def col_to(d):
        return lax.rem(c + d, C)

    def z_to(d):
        return 2 * lax.rem(z + d, Z) + core

    def z_from(d):
        return 2 * lax.rem(z + Z - d, Z) + core

    def rows(at, size):
        return pl.ds(pl.multiple_of(at * size, size), size)

    def rcopy(src, dst, cat, recv, **dev):
        return pltpu.make_async_remote_copy(
            src_ref=src, dst_ref=dst, send_sem=send.at[cat], recv_sem=recv,
            device_id=dev, device_id_type=MESH,
        )

    barrier = pltpu.get_barrier_semaphore()
    for d in range(1, R):
        pl.semaphore_signal(barrier, inc=1, device_id={"row": row_to(d)}, device_id_type=MESH)
    for d in range(1, C):
        pl.semaphore_signal(barrier, inc=1, device_id={"col": col_to(d)}, device_id_type=MESH)
    pl.semaphore_wait(barrier, R + C - 2)

    def g_block(l, at, which):
        return G.at[l, rows(2 * at + which, TR)]

    def g_own(l, step):
        if step == 0:
            return rcopy(grads.at[l], g_block(l, z, core), 2, g_fw.at[l, z], row=sib)
        return rcopy(grads.at[l], g_block(l, z, core), 0, g_in.at[l, z], row=r + 2 * step)

    def g_pass(l, at, step):
        block = g_block(l, at, core)
        if step == 0:
            return rcopy(block, block, 2, g_fw.at[l, at], row=sib)
        return rcopy(block, block, 0, g_in.at[l, at], row=r + 2 * step)

    def g_own_each(l, act):
        act(g_own(l, 0))

        for step in (1, -1, 2, -2):
            @pl.when(jnp.logical_and(z + step >= 0, z + step < Z))
            def _():
                act(g_own(l, step))

    def g_relay(l, d, act, arrive):
        for step in (1, -1):
            at = z - step * d

            @pl.when(jnp.logical_and(at >= 0, at < Z))
            def _():
                if arrive:
                    rcopy(grads.at[l], g_block(l, at, core), 0, g_in.at[l, at], row=r).wait_recv()

                for far in (2 * step, step) if d % 2 == 0 else ():
                    @pl.when(jnp.logical_and(z + far >= 0, z + far < Z))
                    def _():
                        act(g_pass(l, at, far))

                act(g_pass(l, at, 0))

    def a_copy(l, d):
        return rcopy(acts.at[l], A.at[l, rows(c, TC)], 1, a_in.at[l, d], col=col_to(d))

    def rs_copy(l, d):
        return rcopy(rs_send.at[d, l], rs_recv.at[d, l], 3, rs_in.at[l, d], col=col_to(d))

    def sq_copy(d):
        return rcopy(sq.at[r], sq.at[r], 4, sq_in.at[d], row=row_to(d))

    def dt_copy(l, d):
        return rcopy(dt.at[r, l], dt.at[r, l], 5, dt_in.at[l, d], row=row_to(d))

    def at_z(d):
        return lax.rem(z + d, Z)

    def im_copy(d):
        if d == 0:
            return rcopy(im_send.at[1 - core], im_sib, 6, im_in.at[0], row=sib)
        return rcopy(im_acc.at[at_z(d)], im_recv.at[z], 7, im_in.at[d], row=z_to(d))

    def io_fw_copy(l):
        return rcopy(io_send.at[1 - core, l], io_sib.at[l], 8, io_fw.at[l], row=sib)

    def io_copy(l, d):
        return rcopy(io_acc.at[at_z(d), l], io_recv.at[z, l], 9, io_in.at[l, d], row=z_to(d))

    def og_copy(d):
        return rcopy(og.at[r], og.at[r], 11, og_in.at[d], row=sib if d == 0 else z_to(d))

    def og_fw_copy(d):
        return rcopy(og.at[z_from(d)], og.at[z_from(d)], 12, og_fw.at[d], row=sib)

    def q_copy(d):
        return rcopy(q, q_recv.at[d], 10, q_in.at[d], col=col_to(d))

    loads[0].wait()
    loads[1].wait()

    @pl.loop(0, L)
    def _(l):
        @pl.when(l < ahead)
        def _():
            g_own_each(l, lambda copy: copy.start())

        for d in range(1, C):
            a_copy(l, d).start()

    for copy in loads[2:]:
        copy.wait()

    @pl.loop(0, L)
    def _(l):
        G[l, rows(r, TR)] = grads[l]
        A[l, rows(c, TC)] = acts[l]
        m = frozen[l].astype(F32) + mm(ain[l], aout[l], ((0,), (0,)))
        merged[l] = m
        low = m.astype(BF16)
        wlow[l] = low
        sq[r, l] = jnp.sum(m * m, axis=0, keepdims=True)
        inner = mm(ain[l], low, ((1,), (0,)))
        for s in range(R):
            im_send[s % 2, s // 2, l] = inner[s * k:(s + 1) * k]

    for d in range(1, R):
        sq_copy(d).start()
    im_copy(0).start()
    if ahead < L:
        g_own_each(ahead, lambda copy: copy.start())
    for l in range(L):
        mag3[l] = mag[l:l + 1]
    for d in range(1, R):
        rcopy(sq.at[r], sq.at[row_from(d)], 4, sq_in.at[d], row=r).wait_recv()
    total = sq[0]
    for s in range(1, R):
        total = total + sq[s]
    scl[...] = mag3[...] / jnp.sqrt(total + 0.25)
    def pass_on(l):
        rcopy(io_sib.at[l], io_sib.at[l], 8, io_fw.at[l], row=sib).wait_recv()
        for s in range(Z):
            io_acc[s, l] = io_send[core, l, s] + io_sib[l, s]
        for d in range(1, Z):
            io_copy(l, d).start()
        io_recv[z, l] = io_acc[z, l]

    def compute(l):
        for at in range(Z):
            rcopy(grads.at[l], g_block(l, at, 1 - core), 2, g_fw.at[l, at], row=r).wait_recv()
        scale = scl[l]
        g = G[l]
        scaled = (g.astype(F32) * scale).astype(BF16)
        prod[...] = mm(scaled, wlow[l], ((1,), (1,)))
        for d in range(1, C):
            rs_send[d, l] = prod[rows(col_to(d), TC)].astype(BF16)
            rs_copy(l, d).start()
        own[l] = prod[rows(c, TC)]
        for d in range(1, C):
            src = lax.rem(c + C - d, C)
            rcopy(acts.at[l], A.at[l, rows(src, TC)], 1, a_in.at[l, d], col=c).wait_recv()
        outer = mm(A[l], g, ((0,), (0,)))
        dt[r, l] = jnp.sum(merged[l] * outer, axis=0, keepdims=True)
        for d in range(1, R):
            dt_copy(l, d).start()
        inner = mm(ain[l], outer.astype(BF16), ((1,), (0,)))
        for s in range(R):
            io_send[s % 2, l, s // 2] = inner[s * k:(s + 1) * k]
        io_fw_copy(l).start()

        @pl.when(l > 0)
        def _():
            pass_on(l - 1)

        ing[l] = mm(aout[l], (outer * scale).astype(BF16), ((1,), (1,)))

    @pl.loop(0, L + skew)
    def _(at):
        @pl.when(at + ahead + 1 < L)
        def _():
            g_own_each(at + ahead + 1, lambda copy: copy.start())

        for d in range(1, Z):
            l = at - (d - 1) // 2

            @pl.when(jnp.logical_and(l >= 0, l < L))
            def _():
                g_relay(l, d, lambda copy: copy.start(), True)

        @pl.when(at == L - 1)
        def _():
            im_copy(0).wait_recv()
            im_acc[...] = im_send[core] + im_sib[...]
            for d in range(1, Z):
                im_copy(d).start()
            im_recv[z] = im_acc[z]

        @pl.when(at >= skew)
        def _():
            compute(at - skew)

    pass_on(L - 1)

    @pl.loop(0, L)
    def _(l):
        for d in range(1, R):
            rcopy(dt.at[r, l], dt.at[row_from(d), l], 5, dt_in.at[l, d], row=r).wait_recv()

    dots = dt[0]
    for s in range(1, R):
        dots = dots + dt[s]
    norms = jnp.sqrt(total + 0.25)
    ratio = dots / norms
    for l in range(L):
        mgrad[l:l + 1] = ratio[l]
    saves[0].start()
    cor[...] = -mag3[...] * dots / (norms * norms * norms)

    @pl.loop(0, L)
    def _(l):
        adjusted = (merged[l] * cor[l]).astype(BF16)
        part = ing[l] + mm(aout[l], adjusted, ((1,), (1,)))
        ing[l] = part
        q[l] = part.astype(BF16)

    for d in range(1, C):
        q_copy(d).start()
    for d in range(1, Z):
        src = lax.rem(z + Z - d, Z)
        rcopy(im_recv.at[z], im_recv.at[src], 7, im_in.at[d], row=r).wait_recv()

    @pl.loop(0, L)
    def _(l):
        for d in range(1, Z):
            src = lax.rem(z + Z - d, Z)
            rcopy(io_recv.at[z, l], io_recv.at[src, l], 9, io_in.at[l, d], row=r).wait_recv()
        summed, side = io_recv[0, l], im_recv[0, l]
        for s in range(1, Z):
            summed = summed + io_recv[s, l]
            side = side + im_recv[s, l]
        og[r, l] = summed * scl[l] + side * cor[l]

    for d in range(Z):
        og_copy(d).start()

    @pl.loop(0, L)
    def _(l):
        result = own[l]
        for d in range(1, C):
            rcopy(rs_send.at[d, l], rs_recv.at[d, l], 3, rs_in.at[l, d], col=c).wait_recv()
            result = result + rs_recv[d, l].astype(F32)
        ig[l] = result.astype(BF16)

    saves[1].start()

    for d in range(1, C):
        rcopy(q, q_recv.at[d], 10, q_in.at[d], col=c).wait_recv()

    @pl.loop(0, L)
    def _(l):
        result = ing[l]
        for d in range(1, C):
            result = result + q_recv[d, l].astype(F32)
        ing[l] = result

    saves[2].start()

    for d in range(1, Z):
        rcopy(og.at[r], og.at[z_from(d)], 11, og_in.at[d], row=r).wait_recv()
        og_fw_copy(d).start()
    rcopy(og.at[r], og.at[sib], 11, og_in.at[0], row=r).wait_recv()
    for d in range(1, Z):
        from_sib = 2 * lax.rem(z + Z - d, Z) + 1 - core
        rcopy(og.at[r], og.at[from_sib], 12, og_fw.at[d], row=r).wait_recv()

    @pl.loop(0, L)
    def _(l):
        for s in range(R):
            oug[l, s * k:(s + 1) * k] = og[s, l]

    saves[3].start()

    @pl.loop(0, L)
    def _(l):
        g_own_each(l, lambda copy: copy.wait_send())
        for d in range(1, Z):
            g_relay(l, d, lambda copy: copy.wait_send(), False)
        for d in range(1, C):
            a_copy(l, d).wait_send()
            rs_copy(l, d).wait_send()

    @pl.loop(0, L)
    def _(l):
        for d in range(1, R):
            dt_copy(l, d).wait_send()
        io_fw_copy(l).wait_send()
        for d in range(1, Z):
            io_copy(l, d).wait_send()

    for d in range(1, R):
        sq_copy(d).wait_send()
    for d in range(Z):
        im_copy(d).wait_send()
        og_copy(d).wait_send()
    for d in range(1, Z):
        og_fw_copy(d).wait_send()
    for d in range(1, C):
        q_copy(d).wait_send()
    for copy in saves:
        copy.wait()


def finish(ig, ing, oug, mgrad, ig_out, ing_out, oug_out, mgrad_out):
    ig_out[...] = ig[...]
    ing_out[...] = ing[...]
    oug_out[...] = oug[...]
    mgrad_out[...] = mgrad[...]


def body(R, C, acts, grads, frozen, ain, aout, mag):
    L, TR, W = grads.shape
    TC, KI = acts.shape[1:]
    RANK = ain.shape[1]
    k, T, Z = RANK // R, TR * R, R // 2
    V = pltpu.VMEM
    dma = pltpu.SemaphoreType.DMA
    vm = pl.BlockSpec(memory_space=pltpu.VMEM)
    hbm = pl.BlockSpec(memory_space=pltpu.HBM)
    ig, ing, oug, mgrad = pl.pallas_call(
        functools.partial(kernel, R, C),
        out_shape=(
            jax.ShapeDtypeStruct((L, TC, KI), BF16),
            jax.ShapeDtypeStruct((L, RANK, KI), F32),
            jax.ShapeDtypeStruct((L, RANK, W), F32),
            jax.ShapeDtypeStruct((L, W), F32),
        ),
        in_specs=[hbm] * 6,
        out_specs=(hbm,) * 4,
        scratch_shapes=[
            V(acts.shape, BF16), V(grads.shape, BF16), V(frozen.shape, BF16),
            V(ain.shape, BF16), V(aout.shape, BF16), V(mag.shape, F32),
            V((L, TC, KI), BF16), V((L, RANK, KI), F32), V((L, RANK, W), F32), V((L, W), F32),
            dma((6,)), dma((4,)),
            V((L, T, W), BF16), V((L, T, KI), BF16), V((L, KI, W), F32), V((L, KI, W), BF16),
            V((T, KI), F32), V((L, TC, KI), F32), V((C, L, TC, KI), BF16), V((C, L, TC, KI), BF16),
            V((R, L, 1, W), F32), V((R, L, 1, W), F32),
            V((2, Z, L, k, W), F32), V((Z, L, k, W), F32), V((Z, L, k, W), F32), V((Z, L, k, W), F32),
            V((2, L, Z, k, W), F32), V((L, Z, k, W), F32), V((Z, L, k, W), F32), V((Z, L, k, W), F32),
            V((R, L, k, W), F32), V((L, RANK, KI), BF16), V((C, L, RANK, KI), BF16),
            V((L, 1, W), F32), V((L, 1, W), F32), V((L, 1, W), F32),
            dma((13,)), dma((L, Z)), dma((L, Z)), dma((L, C)), dma((L, C)),
            dma((R,)), dma((L, R)), dma((Z,)), dma((L, Z)), dma((L,)), dma((Z,)), dma((Z,)), dma((C,)),
        ],
        compiler_params=pltpu.CompilerParams(
            collective_id=0, has_side_effects=True, vmem_limit_bytes=60 * 1024 * 1024
        ),
    )(acts, grads, frozen, ain, aout, mag)
    return pl.pallas_call(
        finish,
        out_shape=tuple(jax.ShapeDtypeStruct(x.shape, x.dtype) for x in (ig, ing, oug, mgrad)),
        in_specs=[vm] * 4,
        out_specs=(vm,) * 4,
    )(ig, ing, oug, mgrad)


def solution(mesh):
    return jax.shard_map(
        functools.partial(body, mesh.shape["row"], mesh.shape["col"]),
        mesh=mesh,
        in_specs=(
            P(None, "col", "row"),
            P(None, "row", "col"),
            P(None, "row", "col"),
            P(None, None, "row"),
            P(None, None, "col"),
            P(None, "col"),
        ),
        out_specs=(
            P(None, "col", "row"),
            P(None, None, "row"),
            P(None, None, "col"),
            P(None, "col"),
        ),
        check_vma=False,
    )
```

```python
import functools

import jax
import jax.numpy as jnp
from jax import lax
from jax.experimental import pallas as pl
from jax.experimental.pallas import tpu as pltpu
from jax.sharding import PartitionSpec as P

MESH = pl.DeviceIdType.MESH
F32 = jnp.float32
BF16 = jnp.bfloat16


def mm(a, b, dims):
    return lax.dot_general(a, b, (dims, ((), ())), preferred_element_type=F32)


def kernel(
    R, C,
    acts_hbm, grads_hbm, frozen_hbm, ain_hbm, aout_hbm, mag_hbm,
    ig_hbm, ing_hbm, oug_hbm, mgrad_hbm,
    acts, grads, frozen, ain, aout, mag,
    ig, ing, oug, mgrad, load, save,
    G, A, merged, wlow, prod, own, rs_send, rs_recv,
    sq, dt, im_send, im_sib, im_acc, im_recv, io_send, io_sib, io_acc, io_recv, og, q, q_recv,
    scl, cor, mag3, send, g_in, g_fw, a_in, rs_in, sq_in, dt_in, im_in, io_in, io_fw, og_in, og_fw, q_in,
):
    pairs = ((grads_hbm, grads), (acts_hbm, acts), (frozen_hbm, frozen),
             (ain_hbm, ain), (aout_hbm, aout), (mag_hbm, mag))
    loads = [pltpu.make_async_copy(a, b, load.at[i]) for i, (a, b) in enumerate(pairs)]
    for copy in loads:
        copy.start()
    pairs = ((mgrad, mgrad_hbm), (ig, ig_hbm), (ing, ing_hbm), (oug, oug_hbm))
    saves = [pltpu.make_async_copy(a, b, save.at[i]) for i, (a, b) in enumerate(pairs)]
    L, TR, W = grads.shape
    TC, KI = acts.shape[1:]
    RANK = ain.shape[1]
    k = RANK // R
    Z = R // 2
    ahead = min(4, L)
    r, c = lax.axis_index("row"), lax.axis_index("col")
    z, core = r // 2, lax.rem(r, 2)
    sib = 2 * z + 1 - core

    def row_to(d):
        return lax.rem(r + d, R)

    def row_from(d):
        return lax.rem(r + R - d, R)

    def col_to(d):
        return lax.rem(c + d, C)

    def z_to(d):
        return 2 * lax.rem(z + d, Z) + core

    def z_from(d):
        return 2 * lax.rem(z + Z - d, Z) + core

    def rows(at, size):
        return pl.ds(pl.multiple_of(at * size, size), size)

    def rcopy(src, dst, cat, recv, **dev):
        return pltpu.make_async_remote_copy(
            src_ref=src, dst_ref=dst, send_sem=send.at[cat], recv_sem=recv,
            device_id=dev, device_id_type=MESH,
        )

    barrier = pltpu.get_barrier_semaphore()
    for d in range(1, R):
        pl.semaphore_signal(barrier, inc=1, device_id={"row": row_to(d)}, device_id_type=MESH)
    for d in range(1, C):
        pl.semaphore_signal(barrier, inc=1, device_id={"col": col_to(d)}, device_id_type=MESH)
    pl.semaphore_wait(barrier, R + C - 2)

    def g_block(l, at, which):
        return G.at[l, rows(2 * at + which, TR)]

    def g_own(l, step):
        if step == 0:
            return rcopy(grads.at[l], g_block(l, z, core), 2, g_fw.at[l, z], row=sib)
        return rcopy(grads.at[l], g_block(l, z, core), 0, g_in.at[l, z], row=r + 2 * step)

    def g_pass(l, at, step):
        block = g_block(l, at, core)
        if step == 0:
            return rcopy(block, block, 2, g_fw.at[l, at], row=sib)
        return rcopy(block, block, 0, g_in.at[l, at], row=r + 2 * step)

    def g_own_each(l, act):
        act(g_own(l, 0))

        @pl.when(z < Z - 1)
        def _():
            act(g_own(l, 1))

        @pl.when(z > 0)
        def _():
            act(g_own(l, -1))

    def g_relay(l, d, act, arrive):
        for step in (1, -1):
            at = z - step * d

            @pl.when(jnp.logical_and(at >= 0, at < Z))
            def _():
                if arrive:
                    rcopy(grads.at[l], g_block(l, at, core), 0, g_in.at[l, at], row=r).wait_recv()

                @pl.when(jnp.logical_and(z + step >= 0, z + step < Z))
                def _():
                    act(g_pass(l, at, step))

                act(g_pass(l, at, 0))

    def a_copy(l, d):
        return rcopy(acts.at[l], A.at[l, rows(c, TC)], 1, a_in.at[l, d], col=col_to(d))

    def rs_copy(l, d):
        return rcopy(rs_send.at[d, l], rs_recv.at[d, l], 3, rs_in.at[l, d], col=col_to(d))

    def sq_copy(d):
        return rcopy(sq.at[r], sq.at[r], 4, sq_in.at[d], row=row_to(d))

    def dt_copy(l, d):
        return rcopy(dt.at[r, l], dt.at[r, l], 5, dt_in.at[l, d], row=row_to(d))

    def at_z(d):
        return lax.rem(z + d, Z)

    def im_copy(d):
        if d == 0:
            return rcopy(im_send.at[1 - core], im_sib, 6, im_in.at[0], row=sib)
        return rcopy(im_acc.at[at_z(d)], im_recv.at[z], 7, im_in.at[d], row=z_to(d))

    def io_fw_copy(l):
        return rcopy(io_send.at[1 - core, l], io_sib.at[l], 8, io_fw.at[l], row=sib)

    def io_copy(l, d):
        return rcopy(io_acc.at[at_z(d), l], io_recv.at[z, l], 9, io_in.at[l, d], row=z_to(d))

    def og_copy(d):
        return rcopy(og.at[r], og.at[r], 11, og_in.at[d], row=sib if d == 0 else z_to(d))

    def og_fw_copy(d):
        return rcopy(og.at[z_from(d)], og.at[z_from(d)], 12, og_fw.at[d], row=sib)

    def q_copy(d):
        return rcopy(q, q_recv.at[d], 10, q_in.at[d], col=col_to(d))

    loads[0].wait()
    loads[1].wait()

    @pl.loop(0, L)
    def _(l):
        @pl.when(l < ahead)
        def _():
            g_own_each(l, lambda copy: copy.start())

        for d in range(1, C):
            a_copy(l, d).start()

    for copy in loads[2:]:
        copy.wait()

    @pl.loop(0, L)
    def _(l):
        G[l, rows(r, TR)] = grads[l]
        A[l, rows(c, TC)] = acts[l]
        m = frozen[l].astype(F32) + mm(ain[l], aout[l], ((0,), (0,)))
        merged[l] = m
        low = m.astype(BF16)
        wlow[l] = low
        sq[r, l] = jnp.sum(m * m, axis=0, keepdims=True)
        inner = mm(ain[l], low, ((1,), (0,)))
        for s in range(R):
            im_send[s % 2, s // 2, l] = inner[s * k:(s + 1) * k]

    for d in range(1, R):
        sq_copy(d).start()
    im_copy(0).start()
    for l in range(L):
        mag3[l] = mag[l:l + 1]
    if ahead < L:
        g_own_each(ahead, lambda copy: copy.start())

    def scales_ready():
        for d in range(1, R):
            rcopy(sq.at[r], sq.at[row_from(d)], 4, sq_in.at[d], row=r).wait_recv()
        total = sq[0]
        for s in range(1, R):
            total = total + sq[s]
        norms = jnp.sqrt(total + 0.25)
        cor[...] = norms
        scl[...] = mag3[...] / norms

    def pass_on(l):
        rcopy(io_sib.at[l], io_sib.at[l], 8, io_fw.at[l], row=sib).wait_recv()
        for s in range(Z):
            io_acc[s, l] = io_send[core, l, s] + io_sib[l, s]
        for d in range(1, Z):
            io_copy(l, d).start()
        io_recv[z, l] = io_acc[z, l]

    def compute(l):
        for at in range(Z):
            rcopy(grads.at[l], g_block(l, at, 1 - core), 2, g_fw.at[l, at], row=r).wait_recv()
        scale = scl[l]
        g = G[l]
        scaled = (g.astype(F32) * scale).astype(BF16)
        prod[...] = mm(scaled, wlow[l], ((1,), (1,)))
        for d in range(1, C):
            rs_send[d, l] = prod[rows(col_to(d), TC)].astype(BF16)
            rs_copy(l, d).start()
        own[l] = prod[rows(c, TC)]
        for d in range(1, C):
            src = lax.rem(c + C - d, C)
            rcopy(acts.at[l], A.at[l, rows(src, TC)], 1, a_in.at[l, d], col=c).wait_recv()
        outer = mm(A[l], g, ((0,), (0,)))
        dt[r, l] = jnp.sum(merged[l] * outer, axis=0, keepdims=True)
        for d in range(1, R):
            dt_copy(l, d).start()
        inner = mm(ain[l], outer.astype(BF16), ((1,), (0,)))
        for s in range(R):
            io_send[s % 2, l, s // 2] = inner[s * k:(s + 1) * k]
        io_fw_copy(l).start()

        @pl.when(l > 0)
        def _():
            pass_on(l - 1)

        ing[l] = mm(aout[l], (outer * scale).astype(BF16), ((1,), (1,)))

    @pl.loop(0, L + Z - 1)
    def _(at):
        @pl.when(at + ahead + 1 < L)
        def _():
            g_own_each(at + ahead + 1, lambda copy: copy.start())

        for d in range(1, Z):
            l = at - (d - 1)

            @pl.when(jnp.logical_and(l >= 0, l < L))
            def _():
                g_relay(l, d, lambda copy: copy.start(), True)

        @pl.when(at == L + Z - 3)
        def _():
            im_copy(0).wait_recv()
            im_acc[...] = im_send[core] + im_sib[...]
            for d in range(1, Z):
                im_copy(d).start()
            im_recv[z] = im_acc[z]

        @pl.when(at == Z - 1)
        def _():
            scales_ready()

        @pl.when(at >= Z - 1)
        def _():
            compute(at - (Z - 1))

    pass_on(L - 1)

    @pl.loop(0, L)
    def _(l):
        for d in range(1, R):
            rcopy(dt.at[r, l], dt.at[row_from(d), l], 5, dt_in.at[l, d], row=r).wait_recv()

    dots = dt[0]
    for s in range(1, R):
        dots = dots + dt[s]
    norms = cor[...]
    ratio = dots / norms
    for l in range(L):
        mgrad[l:l + 1] = ratio[l]
    saves[0].start()
    cor[...] = -mag3[...] * dots / (norms * norms * norms)

    @pl.loop(0, L)
    def _(l):
        adjusted = (merged[l] * cor[l]).astype(BF16)
        part = ing[l] + mm(aout[l], adjusted, ((1,), (1,)))
        ing[l] = part
        q[l] = part.astype(BF16)

    for d in range(1, C):
        q_copy(d).start()
    for d in range(1, Z):
        src = lax.rem(z + Z - d, Z)
        rcopy(im_recv.at[z], im_recv.at[src], 7, im_in.at[d], row=r).wait_recv()

    @pl.loop(0, L)
    def _(l):
        for d in range(1, Z):
            src = lax.rem(z + Z - d, Z)
            rcopy(io_recv.at[z, l], io_recv.at[src, l], 9, io_in.at[l, d], row=r).wait_recv()
        summed, side = io_recv[0, l], im_recv[0, l]
        for s in range(1, Z):
            summed = summed + io_recv[s, l]
            side = side + im_recv[s, l]
        og[r, l] = summed * scl[l] + side * cor[l]

    for d in range(Z):
        og_copy(d).start()

    @pl.loop(0, L)
    def _(l):
        result = own[l]
        for d in range(1, C):
            rcopy(rs_send.at[d, l], rs_recv.at[d, l], 3, rs_in.at[l, d], col=c).wait_recv()
            result = result + rs_recv[d, l].astype(F32)
        ig[l] = result.astype(BF16)

    saves[1].start()

    for d in range(1, C):
        rcopy(q, q_recv.at[d], 10, q_in.at[d], col=c).wait_recv()

    @pl.loop(0, L)
    def _(l):
        result = ing[l]
        for d in range(1, C):
            result = result + q_recv[d, l].astype(F32)
        ing[l] = result

    saves[2].start()

    for d in range(1, Z):
        rcopy(og.at[r], og.at[z_from(d)], 11, og_in.at[d], row=r).wait_recv()
        og_fw_copy(d).start()
    rcopy(og.at[r], og.at[sib], 11, og_in.at[0], row=r).wait_recv()
    for d in range(1, Z):
        from_sib = 2 * lax.rem(z + Z - d, Z) + 1 - core
        rcopy(og.at[r], og.at[from_sib], 12, og_fw.at[d], row=r).wait_recv()

    @pl.loop(0, L)
    def _(l):
        for s in range(R):
            oug[l, s * k:(s + 1) * k] = og[s, l]

    saves[3].start()

    @pl.loop(0, L)
    def _(l):
        g_own_each(l, lambda copy: copy.wait_send())
        for d in range(1, Z):
            g_relay(l, d, lambda copy: copy.wait_send(), False)
        for d in range(1, C):
            a_copy(l, d).wait_send()
            rs_copy(l, d).wait_send()

    @pl.loop(0, L)
    def _(l):
        for d in range(1, R):
            dt_copy(l, d).wait_send()
        io_fw_copy(l).wait_send()
        for d in range(1, Z):
            io_copy(l, d).wait_send()

    for d in range(1, R):
        sq_copy(d).wait_send()
    for d in range(Z):
        im_copy(d).wait_send()
        og_copy(d).wait_send()
    for d in range(1, Z):
        og_fw_copy(d).wait_send()
    for d in range(1, C):
        q_copy(d).wait_send()
    for copy in saves:
        copy.wait()


def finish(ig, ing, oug, mgrad, ig_out, ing_out, oug_out, mgrad_out):
    ig_out[...] = ig[...]
    ing_out[...] = ing[...]
    oug_out[...] = oug[...]
    mgrad_out[...] = mgrad[...]


def body(R, C, acts, grads, frozen, ain, aout, mag):
    L, TR, W = grads.shape
    TC, KI = acts.shape[1:]
    RANK = ain.shape[1]
    k, T, Z = RANK // R, TR * R, R // 2
    V = pltpu.VMEM
    dma = pltpu.SemaphoreType.DMA
    vm = pl.BlockSpec(memory_space=pltpu.VMEM)
    hbm = pl.BlockSpec(memory_space=pltpu.HBM)
    ig, ing, oug, mgrad = pl.pallas_call(
        functools.partial(kernel, R, C),
        out_shape=(
            jax.ShapeDtypeStruct((L, TC, KI), BF16),
            jax.ShapeDtypeStruct((L, RANK, KI), F32),
            jax.ShapeDtypeStruct((L, RANK, W), F32),
            jax.ShapeDtypeStruct((L, W), F32),
        ),
        in_specs=[hbm] * 6,
        out_specs=(hbm,) * 4,
        scratch_shapes=[
            V(acts.shape, BF16), V(grads.shape, BF16), V(frozen.shape, BF16),
            V(ain.shape, BF16), V(aout.shape, BF16), V(mag.shape, F32),
            V((L, TC, KI), BF16), V((L, RANK, KI), F32), V((L, RANK, W), F32), V((L, W), F32),
            dma((6,)), dma((4,)),
            V((L, T, W), BF16), V((L, T, KI), BF16), V((L, KI, W), F32), V((L, KI, W), BF16),
            V((T, KI), F32), V((L, TC, KI), F32), V((C, L, TC, KI), BF16), V((C, L, TC, KI), BF16),
            V((R, L, 1, W), F32), V((R, L, 1, W), F32),
            V((2, Z, L, k, W), F32), V((Z, L, k, W), F32), V((Z, L, k, W), F32), V((Z, L, k, W), F32),
            V((2, L, Z, k, W), F32), V((L, Z, k, W), F32), V((Z, L, k, W), F32), V((Z, L, k, W), F32),
            V((R, L, k, W), F32), V((L, RANK, KI), BF16), V((C, L, RANK, KI), BF16),
            V((L, 1, W), F32), V((L, 1, W), F32), V((L, 1, W), F32),
            dma((13,)), dma((L, Z)), dma((L, Z)), dma((L, C)), dma((L, C)),
            dma((R,)), dma((L, R)), dma((Z,)), dma((L, Z)), dma((L,)), dma((Z,)), dma((Z,)), dma((C,)),
        ],
        compiler_params=pltpu.CompilerParams(
            collective_id=0, has_side_effects=True, vmem_limit_bytes=60 * 1024 * 1024
        ),
    )(acts, grads, frozen, ain, aout, mag)
    return pl.pallas_call(
        finish,
        out_shape=tuple(jax.ShapeDtypeStruct(x.shape, x.dtype) for x in (ig, ing, oug, mgrad)),
        in_specs=[vm] * 4,
        out_specs=(vm,) * 4,
    )(ig, ing, oug, mgrad)


def solution(mesh):
    return jax.shard_map(
        functools.partial(body, mesh.shape["row"], mesh.shape["col"]),
        mesh=mesh,
        in_specs=(
            P(None, "col", "row"),
            P(None, "row", "col"),
            P(None, "row", "col"),
            P(None, None, "row"),
            P(None, None, "col"),
            P(None, "col"),
        ),
        out_specs=(
            P(None, "col", "row"),
            P(None, None, "row"),
            P(None, None, "col"),
            P(None, "col"),
        ),
        check_vma=False,
    )
```

```python
import functools

import jax
import jax.numpy as jnp
from jax import lax
from jax.experimental import pallas as pl
from jax.experimental.pallas import tpu as pltpu
from jax.sharding import PartitionSpec as P

MESH = pl.DeviceIdType.MESH
F32 = jnp.float32
BF16 = jnp.bfloat16


def mm(a, b, dims):
    return lax.dot_general(a, b, (dims, ((), ())), preferred_element_type=F32)


def kernel(
    R, C,
    acts_hbm, grads_hbm, frozen_hbm, ain_hbm, aout_hbm, mag_hbm,
    ig_hbm, ing_hbm, oug_hbm, mgrad_hbm,
    acts, grads, frozen, ain, aout, mag,
    ig, ing, oug, mgrad, load, save,
    G, A, merged, wlow, prod, own, rs_send, rs_recv,
    sq, dt, im_send, im_sib, im_acc, im_recv, io_send, io_sib, io_acc, io_recv, og, q, q_recv,
    scl, cor, mag3, send, g_in, g_fw, a_in, rs_in, sq_in, dt_in, im_in, io_in, io_fw, og_in, og_fw, q_in,
):
    pairs = ((grads_hbm, grads), (acts_hbm, acts), (frozen_hbm, frozen),
             (ain_hbm, ain), (aout_hbm, aout), (mag_hbm, mag))
    loads = [pltpu.make_async_copy(a, b, load.at[i]) for i, (a, b) in enumerate(pairs)]
    for copy in loads:
        copy.start()
    pairs = ((mgrad, mgrad_hbm), (ig, ig_hbm), (ing, ing_hbm), (oug, oug_hbm))
    saves = [pltpu.make_async_copy(a, b, save.at[i]) for i, (a, b) in enumerate(pairs)]
    L, TR, W = grads.shape
    TC, KI = acts.shape[1:]
    RANK = ain.shape[1]
    k = RANK // R
    Z = R // 2
    ahead = min(4, L)
    r, c = lax.axis_index("row"), lax.axis_index("col")
    z, core = r // 2, lax.rem(r, 2)
    sib = 2 * z + 1 - core

    def row_to(d):
        return lax.rem(r + d, R)

    def row_from(d):
        return lax.rem(r + R - d, R)

    def col_to(d):
        return lax.rem(c + d, C)

    def z_to(d):
        return 2 * lax.rem(z + d, Z) + core

    def z_from(d):
        return 2 * lax.rem(z + Z - d, Z) + core

    def rows(at, size):
        return pl.ds(pl.multiple_of(at * size, size), size)

    def rcopy(src, dst, cat, recv, **dev):
        return pltpu.make_async_remote_copy(
            src_ref=src, dst_ref=dst, send_sem=send.at[cat], recv_sem=recv,
            device_id=dev, device_id_type=MESH,
        )

    barrier = pltpu.get_barrier_semaphore()
    for d in range(1, R):
        pl.semaphore_signal(barrier, inc=1, device_id={"row": row_to(d)}, device_id_type=MESH)
    for d in range(1, C):
        pl.semaphore_signal(barrier, inc=1, device_id={"col": col_to(d)}, device_id_type=MESH)
    pl.semaphore_wait(barrier, R + C - 2)

    def g_block(l, at, which):
        return G.at[l, rows(2 * at + which, TR)]

    def g_own(l, step):
        if step == 0:
            return rcopy(grads.at[l], g_block(l, z, core), 2, g_fw.at[l, z], row=sib)
        return rcopy(grads.at[l], g_block(l, z, core), 0, g_in.at[l, z], row=r + 2 * step)

    def g_pass(l, at, step):
        block = g_block(l, at, core)
        if step == 0:
            return rcopy(block, block, 2, g_fw.at[l, at], row=sib)
        return rcopy(block, block, 0, g_in.at[l, at], row=r + 2 * step)

    def g_own_each(l, act):
        act(g_own(l, 0))

        @pl.when(z < Z - 1)
        def _():
            act(g_own(l, 1))

        @pl.when(z > 0)
        def _():
            act(g_own(l, -1))

    def g_relay(l, d, act, arrive):
        for step in (1, -1):
            at = z - step * d

            @pl.when(jnp.logical_and(at >= 0, at < Z))
            def _():
                if arrive:
                    rcopy(grads.at[l], g_block(l, at, core), 0, g_in.at[l, at], row=r).wait_recv()

                @pl.when(jnp.logical_and(z + step >= 0, z + step < Z))
                def _():
                    act(g_pass(l, at, step))

                act(g_pass(l, at, 0))

    def a_copy(l, d):
        return rcopy(acts.at[l], A.at[l, rows(c, TC)], 1, a_in.at[l, d], col=col_to(d))

    def rs_copy(l, d):
        return rcopy(rs_send.at[d, l], rs_recv.at[d, l], 3, rs_in.at[l, d], col=col_to(d))

    def sq_copy(d):
        return rcopy(sq.at[r], sq.at[r], 4, sq_in.at[d], row=row_to(d))

    def dt_copy(l, d):
        return rcopy(dt.at[r, l], dt.at[r, l], 5, dt_in.at[l, d], row=row_to(d))

    def at_z(d):
        return lax.rem(z + d, Z)

    def im_copy(d):
        if d == 0:
            return rcopy(im_send.at[1 - core], im_sib, 6, im_in.at[0], row=sib)
        return rcopy(im_acc.at[at_z(d)], im_recv.at[z], 7, im_in.at[d], row=z_to(d))

    def io_fw_copy(l):
        return rcopy(io_send.at[1 - core, l], io_sib.at[l], 8, io_fw.at[l], row=sib)

    def io_copy(l, d):
        return rcopy(io_acc.at[at_z(d), l], io_recv.at[z, l], 9, io_in.at[l, d], row=z_to(d))

    def og_copy(d):
        return rcopy(og.at[r], og.at[r], 11, og_in.at[d], row=sib if d == 0 else z_to(d))

    def og_fw_copy(d):
        return rcopy(og.at[z_from(d)], og.at[z_from(d)], 12, og_fw.at[d], row=sib)

    def q_copy(d):
        return rcopy(q, q_recv.at[d], 10, q_in.at[d], col=col_to(d))

    loads[0].wait()
    loads[1].wait()

    @pl.loop(0, L)
    def _(l):
        @pl.when(l < ahead)
        def _():
            g_own_each(l, lambda copy: copy.start())

        for d in range(1, C):
            a_copy(l, d).start()

    for copy in loads[2:]:
        copy.wait()

    @pl.loop(0, L)
    def _(l):
        G[l, rows(r, TR)] = grads[l]
        A[l, rows(c, TC)] = acts[l]
        m = frozen[l].astype(F32) + mm(ain[l], aout[l], ((0,), (0,)))
        merged[l] = m
        low = m.astype(BF16)
        wlow[l] = low
        sq[r, l] = jnp.sum(m * m, axis=0, keepdims=True)
        inner = mm(ain[l], low, ((1,), (0,)))
        for s in range(R):
            im_send[s % 2, s // 2, l] = inner[s * k:(s + 1) * k]

    for d in range(1, R):
        sq_copy(d).start()
    im_copy(0).start()
    for l in range(L):
        mag3[l] = mag[l:l + 1]
    if ahead < L:
        g_own_each(ahead, lambda copy: copy.start())

    def scales_ready():
        for d in range(1, R):
            rcopy(sq.at[r], sq.at[row_from(d)], 4, sq_in.at[d], row=r).wait_recv()
        total = sq[0]
        for s in range(1, R):
            total = total + sq[s]
        norms = jnp.sqrt(total + 0.25)
        cor[...] = norms
        scl[...] = mag3[...] / norms

    def pass_on(l):
        rcopy(io_sib.at[l], io_sib.at[l], 8, io_fw.at[l], row=sib).wait_recv()
        for s in range(Z):
            io_acc[s, l] = io_send[core, l, s] + io_sib[l, s]
        for d in range(1, Z):
            io_copy(l, d).start()
        io_recv[z, l] = io_acc[z, l]

    def compute(l):
        for at in range(Z):
            rcopy(grads.at[l], g_block(l, at, 1 - core), 2, g_fw.at[l, at], row=r).wait_recv()
        scale = scl[l]
        g = G[l]
        scaled = (g.astype(F32) * scale).astype(BF16)
        prod[...] = mm(scaled, wlow[l], ((1,), (1,)))
        for d in range(1, C):
            rs_send[d, l] = prod[rows(col_to(d), TC)].astype(BF16)
            rs_copy(l, d).start()
        own[l] = prod[rows(c, TC)]
        for d in range(1, C):
            src = lax.rem(c + C - d, C)
            rcopy(acts.at[l], A.at[l, rows(src, TC)], 1, a_in.at[l, d], col=c).wait_recv()
        outer = mm(A[l], g, ((0,), (0,)))
        dt[r, l] = jnp.sum(merged[l] * outer, axis=0, keepdims=True)
        for d in range(1, R):
            dt_copy(l, d).start()
        inner = mm(ain[l], outer.astype(BF16), ((1,), (0,)))
        for s in range(R):
            io_send[s % 2, l, s // 2] = inner[s * k:(s + 1) * k]
        io_fw_copy(l).start()

        @pl.when(l > 0)
        def _():
            pass_on(l - 1)

        ing[l] = mm(aout[l], (outer * scale).astype(BF16), ((1,), (1,)))

    @pl.loop(0, L + Z - 2)
    def _(at):
        @pl.when(at + ahead + 1 < L)
        def _():
            g_own_each(at + ahead + 1, lambda copy: copy.start())

        for d in range(1, Z):
            l = at - (d - 1)

            @pl.when(jnp.logical_and(l >= 0, l < L))
            def _():
                g_relay(l, d, lambda copy: copy.start(), True)

        @pl.when(at == L + Z - 3)
        def _():
            im_copy(0).wait_recv()
            im_acc[...] = im_send[core] + im_sib[...]
            for d in range(1, Z):
                im_copy(d).start()
            im_recv[z] = im_acc[z]

        @pl.when(at == Z - 2)
        def _():
            scales_ready()

        @pl.when(at >= Z - 2)
        def _():
            compute(at - (Z - 2))

    pass_on(L - 1)

    @pl.loop(0, L)
    def _(l):
        for d in range(1, R):
            rcopy(dt.at[r, l], dt.at[row_from(d), l], 5, dt_in.at[l, d], row=r).wait_recv()

    dots = dt[0]
    for s in range(1, R):
        dots = dots + dt[s]
    norms = cor[...]
    ratio = dots / norms
    for l in range(L):
        mgrad[l:l + 1] = ratio[l]
    saves[0].start()
    cor[...] = -mag3[...] * dots / (norms * norms * norms)

    @pl.loop(0, L)
    def _(l):
        adjusted = (merged[l] * cor[l]).astype(BF16)
        part = ing[l] + mm(aout[l], adjusted, ((1,), (1,)))
        ing[l] = part
        q[l] = part.astype(BF16)

    for d in range(1, C):
        q_copy(d).start()
    for d in range(1, Z):
        src = lax.rem(z + Z - d, Z)
        rcopy(im_recv.at[z], im_recv.at[src], 7, im_in.at[d], row=r).wait_recv()

    @pl.loop(0, L)
    def _(l):
        for d in range(1, Z):
            src = lax.rem(z + Z - d, Z)
            rcopy(io_recv.at[z, l], io_recv.at[src, l], 9, io_in.at[l, d], row=r).wait_recv()
        summed, side = io_recv[0, l], im_recv[0, l]
        for s in range(1, Z):
            summed = summed + io_recv[s, l]
            side = side + im_recv[s, l]
        og[r, l] = summed * scl[l] + side * cor[l]

    for d in range(Z):
        og_copy(d).start()

    @pl.loop(0, L)
    def _(l):
        result = own[l]
        for d in range(1, C):
            rcopy(rs_send.at[d, l], rs_recv.at[d, l], 3, rs_in.at[l, d], col=c).wait_recv()
            result = result + rs_recv[d, l].astype(F32)
        ig[l] = result.astype(BF16)

    saves[1].start()

    for d in range(1, C):
        rcopy(q, q_recv.at[d], 10, q_in.at[d], col=c).wait_recv()

    @pl.loop(0, L)
    def _(l):
        result = ing[l]
        for d in range(1, C):
            result = result + q_recv[d, l].astype(F32)
        ing[l] = result

    saves[2].start()

    for d in range(1, Z):
        rcopy(og.at[r], og.at[z_from(d)], 11, og_in.at[d], row=r).wait_recv()
        og_fw_copy(d).start()
    rcopy(og.at[r], og.at[sib], 11, og_in.at[0], row=r).wait_recv()
    for d in range(1, Z):
        from_sib = 2 * lax.rem(z + Z - d, Z) + 1 - core
        rcopy(og.at[r], og.at[from_sib], 12, og_fw.at[d], row=r).wait_recv()

    @pl.loop(0, L)
    def _(l):
        for s in range(R):
            oug[l, s * k:(s + 1) * k] = og[s, l]

    saves[3].start()

    @pl.loop(0, L)
    def _(l):
        g_own_each(l, lambda copy: copy.wait_send())
        for d in range(1, Z):
            g_relay(l, d, lambda copy: copy.wait_send(), False)
        for d in range(1, C):
            a_copy(l, d).wait_send()
            rs_copy(l, d).wait_send()

    @pl.loop(0, L)
    def _(l):
        for d in range(1, R):
            dt_copy(l, d).wait_send()
        io_fw_copy(l).wait_send()
        for d in range(1, Z):
            io_copy(l, d).wait_send()

    for d in range(1, R):
        sq_copy(d).wait_send()
    for d in range(Z):
        im_copy(d).wait_send()
        og_copy(d).wait_send()
    for d in range(1, Z):
        og_fw_copy(d).wait_send()
    for d in range(1, C):
        q_copy(d).wait_send()
    for copy in saves:
        copy.wait()


def finish(ig, ing, oug, mgrad, ig_out, ing_out, oug_out, mgrad_out):
    ig_out[...] = ig[...]
    ing_out[...] = ing[...]
    oug_out[...] = oug[...]
    mgrad_out[...] = mgrad[...]


def body(R, C, acts, grads, frozen, ain, aout, mag):
    L, TR, W = grads.shape
    TC, KI = acts.shape[1:]
    RANK = ain.shape[1]
    k, T, Z = RANK // R, TR * R, R // 2
    V = pltpu.VMEM
    dma = pltpu.SemaphoreType.DMA
    vm = pl.BlockSpec(memory_space=pltpu.VMEM)
    hbm = pl.BlockSpec(memory_space=pltpu.HBM)
    ig, ing, oug, mgrad = pl.pallas_call(
        functools.partial(kernel, R, C),
        out_shape=(
            jax.ShapeDtypeStruct((L, TC, KI), BF16),
            jax.ShapeDtypeStruct((L, RANK, KI), F32),
            jax.ShapeDtypeStruct((L, RANK, W), F32),
            jax.ShapeDtypeStruct((L, W), F32),
        ),
        in_specs=[hbm] * 6,
        out_specs=(hbm,) * 4,
        scratch_shapes=[
            V(acts.shape, BF16), V(grads.shape, BF16), V(frozen.shape, BF16),
            V(ain.shape, BF16), V(aout.shape, BF16), V(mag.shape, F32),
            V((L, TC, KI), BF16), V((L, RANK, KI), F32), V((L, RANK, W), F32), V((L, W), F32),
            dma((6,)), dma((4,)),
            V((L, T, W), BF16), V((L, T, KI), BF16), V((L, KI, W), F32), V((L, KI, W), BF16),
            V((T, KI), F32), V((L, TC, KI), F32), V((C, L, TC, KI), BF16), V((C, L, TC, KI), BF16),
            V((R, L, 1, W), F32), V((R, L, 1, W), F32),
            V((2, Z, L, k, W), F32), V((Z, L, k, W), F32), V((Z, L, k, W), F32), V((Z, L, k, W), F32),
            V((2, L, Z, k, W), F32), V((L, Z, k, W), F32), V((Z, L, k, W), F32), V((Z, L, k, W), F32),
            V((R, L, k, W), F32), V((L, RANK, KI), BF16), V((C, L, RANK, KI), BF16),
            V((L, 1, W), F32), V((L, 1, W), F32), V((L, 1, W), F32),
            dma((13,)), dma((L, Z)), dma((L, Z)), dma((L, C)), dma((L, C)),
            dma((R,)), dma((L, R)), dma((Z,)), dma((L, Z)), dma((L,)), dma((Z,)), dma((Z,)), dma((C,)),
        ],
        compiler_params=pltpu.CompilerParams(
            collective_id=0, has_side_effects=True, vmem_limit_bytes=60 * 1024 * 1024
        ),
    )(acts, grads, frozen, ain, aout, mag)
    return pl.pallas_call(
        finish,
        out_shape=tuple(jax.ShapeDtypeStruct(x.shape, x.dtype) for x in (ig, ing, oug, mgrad)),
        in_specs=[vm] * 4,
        out_specs=(vm,) * 4,
    )(ig, ing, oug, mgrad)


def solution(mesh):
    return jax.shard_map(
        functools.partial(body, mesh.shape["row"], mesh.shape["col"]),
        mesh=mesh,
        in_specs=(
            P(None, "col", "row"),
            P(None, "row", "col"),
            P(None, "row", "col"),
            P(None, None, "row"),
            P(None, None, "col"),
            P(None, "col"),
        ),
        out_specs=(
            P(None, "col", "row"),
            P(None, None, "row"),
            P(None, None, "col"),
            P(None, "col"),
        ),
        check_vma=False,
    )
```
